64 devices in a mesh: rep: 4 (over x, y), dp: 16 (over z, core).
Axes of the slice: x: 2, y: 2, z: 8, core: 2. Of those that a mesh axis runs over, the one named last changes fastest.
The devices are a block of a 4x4x8 slice.
Arguments:
- a: bfloat16 [64, 4, 4096, 640], P(('rep', 'dp')), parts along dimension 0
- g: bfloat16 [64, 4, 4096, 2560], P(('rep', 'dp')), parts along dimension 0
Outputs:
- output: bfloat16 [16, 640, 2560], P('rep'), parts along dimension 0
There are 4 independent parts. The reference program is written for one: setup_inputs(seed, part) draws one part's arguments, and reference() takes and returns one part's arrays. A program takes and returns all parts, laid end to end along the dimension named above; each array names one.
All inputs are finite; a program needn't handle non-finite values.
Results may differ from the reference program's by a relative error of at most 0.012.
Values are sent between devices in bfloat16 or wider.
A program may use at most 768 MiB of HBM per device.

```python
import jax
import jax.numpy as jnp
from jax import lax

DEVICES = 16
MATRICES = 4
TOKENS = 4096
D = 640
FF = 2560


def setup_inputs(seed: int = 0, part: int = 0) -> dict:
    ka, kg, ks = (jax.random.fold_in(k, part) for k in jax.random.split(jax.random.key(seed), 3))
    size = 2.0 ** jax.random.uniform(ks, (DEVICES, MATRICES, 1, 1), jnp.float32, -1.0, 1.0)
    a = jax.random.normal(ka, (DEVICES, MATRICES, TOKENS, D), jnp.float32)
    g = size * jax.random.normal(kg, (DEVICES, MATRICES, TOKENS, FF), jnp.float32) * (DEVICES * TOKENS) ** -0.5
    return {"a": a.astype(jnp.bfloat16), "g": g.astype(jnp.bfloat16)}


def reference(a, g):
    def take(so_far, one):
        return so_far + jnp.einsum("ntd,ntf->ndf", *one, preferred_element_type=jnp.float32), None

    return lax.scan(take, jnp.zeros((MATRICES, D, FF), jnp.float32), (a, g))[0].astype(jnp.bfloat16)
```

```python
import functools

import jax
import jax.numpy as jnp
from jax import lax
from jax.experimental import pallas as pl
from jax.experimental.pallas import tpu as pltpu
from jax.sharding import PartitionSpec as P

MESH = pl.DeviceIdType.MESH
F32 = jnp.float32
BF16 = jnp.bfloat16


def sizes(n, a_shape, g_shape):
    mats, tokens, d = a_shape
    ff = g_shape[2]
    chips = n // 2
    assert chips == 2 * mats and mats == 4
    width = ff * mats // chips
    tile = 256 if width % 256 == 0 else 128
    return dict(
        mats=mats, tokens=tokens, d=d, ff=ff, chips=chips, half=d // 2, width=width, tile=tile,
        tiles=width // tile, chunk=tokens // 8, chunks=8,
    )


def sum_kernel(n, s, a_hbm, g_hbm, out, at, araw, gbuf, part, part_half, land, head, psend, acc,
               a_sem, g_sem, ps_sem, pr_sem, rs_send, rs_recv, ag_send, ag_recv, ad_send, ad_recv):
    mats, chips, half, tile, tiles = s["mats"], s["chips"], s["half"], s["tile"], s["tiles"]
    d, width, chunk, chunks = s["d"], s["width"], s["chunk"], s["chunks"]
    far = chips // 2
    depth = gbuf.shape[0]
    me = lax.axis_index("dp")
    core = me % 2
    c = me // 2
    sgn = 2 * core - 1
    nxt = {"dp": ((c + sgn + chips) % chips) * 2 + core}
    prv = {"dp": ((c - sgn + chips) % chips) * 2 + core}
    partner = {"dp": c * 2 + 1 - core}
    mine = pl.multiple_of(core * half, half)
    other = pl.multiple_of((1 - core) * half, half)
    big = 8 * chips

    def shard(r):
        return (c + sgn * r + big) % chips

    def slot_of(r):
        return (r + big) % mats

    def columns(j, i):
        return pl.ds(pl.multiple_of((j // mats) * width + i * tile, tile), tile)

    def a_copy(slot, r):
        m = (c + sgn * slot + big) % mats
        return pltpu.make_async_copy(
            a_hbm.at[m, pl.ds(pl.multiple_of(r * chunk, chunk), chunk)], araw.at[r], a_sem.at[r])

    def g_copy(q, j, i):
        b = q % depth
        return pltpu.make_async_copy(g_hbm.at[j % mats, :, columns(j, i)], gbuf.at[b], g_sem.at[b])

    def g_start(q):
        @pl.when(q < tiles)
        def _():
            g_copy(q, shard(far), q).start()

        @pl.when((q >= tiles) & (q < tiles * 7))
        def _():
            r = q - tiles
            k = 3 - r // (2 * tiles)
            w = r % (2 * tiles)
            g_copy(q, shard(k * (2 * (w % 2) - 1)), w // 2).start()

        @pl.when((q >= tiles * 7) & (q < tiles * 8))
        def _():
            g_copy(q, shard(0), q - tiles * 7).start()

    def g_wait(q):
        g_copy(q, 0, 0).wait()

    def transpose(slot, r):
        a_copy(slot, r).wait()
        at[slot, :, pl.ds(pl.multiple_of(r * chunk, chunk), chunk)] = araw[r].T

    def dot(slot, row, rows, q):
        return jnp.dot(at[slot, pl.ds(row, rows), :], gbuf[q % depth], preferred_element_type=F32)

    def to_partner(src, dst, u, k, i):
        return pltpu.make_async_remote_copy(
            src, dst, ps_sem.at[u], pr_sem.at[k, i], device_id=partner, device_id_type=MESH)

    def full_p(u, k, i):
        return to_partner(psend.at[u], part.at[k - 1, i], u, k, i)

    def half_p(u, k, i):
        return to_partner(psend.at[u, pl.ds(0, half)], part_half.at[k // far, i], u, k, i)

    def rs_head(i):
        return pltpu.make_async_remote_copy(
            head.at[i], land.at[far - 1, i, pl.ds(mine, half)], rs_send.at[far - 1, i],
            rs_recv.at[far - 1, i], device_id=nxt, device_id_type=MESH)

    def rs_full(k, i):
        return pltpu.make_async_remote_copy(
            land.at[k, i], land.at[k - 1, i], rs_send.at[k - 1, i], rs_recv.at[k - 1, i],
            device_id=nxt, device_id_type=MESH)

    def block(ref, j, row, i):
        return ref.at[j % mats, pl.ds(row, half), columns(j, i)]

    def ag(h, i):
        b = block(out, shard(-(h - 1)), mine, i)
        return pltpu.make_async_remote_copy(
            b, b, ag_send.at[h - 1, i], ag_recv.at[h - 1, i], device_id=nxt, device_id_type=MESH)

    def ag_arrival(h, i):
        b = block(out, shard(-h), mine, i)
        return pltpu.make_async_remote_copy(
            b, b, ag_send.at[h - 1, i], ag_recv.at[h - 1, i], device_id=nxt, device_id_type=MESH)

    def across(h, i):
        b = block(out, shard(-h), mine, i)
        return pltpu.make_async_remote_copy(
            b, b, ad_send.at[h, i], ad_recv.at[h, i], device_id=partner, device_id_type=MESH)

    def across_arrival(h, i):
        b = block(out, shard(h), other, i)
        return pltpu.make_async_remote_copy(
            b, b, ad_send.at[h, i], ad_recv.at[h, i], device_id=partner, device_id_type=MESH)

    for r in range(chunks):
        a_copy(0, r).start()
    g_start(0)
    g_start(1)
    barrier = pltpu.get_barrier_semaphore()
    for peer in (nxt, prv, partner):
        pl.semaphore_signal(barrier, 1, device_id=peer, device_id_type=MESH)
    pl.semaphore_wait(barrier, 3)

    def first(r, _):
        transpose(0, r)
        a_copy(1, r).start()
        return 0

    lax.fori_loop(0, chunks, first, 0)

    def head_out(i):
        half_p(i % 2, far, i).wait_recv()
        head[i] = (acc[pl.ds(0, half)] + part_half[1, i].astype(F32)).astype(BF16)
        rs_head(i).start()

    def phase_far(i, _):
        g_start(i + 2)
        g_wait(i)

        @pl.when(i >= 2)
        def _():
            half_p(i % 2, far, i).wait_send()

        psend[i % 2, pl.ds(0, half)] = dot(0, other, half, i).astype(BF16)
        half_p(i % 2, far, i).start()

        @pl.when(i >= 1)
        def _():
            head_out(i - 1)

        acc[pl.ds(0, half)] = dot(0, mine, half, i)

        @pl.when(i < 4)
        def _():
            for u in range(4):
                r = (4 * i + u) % chunks
                transpose(1 + 2 * (i // 2), r)
                a_copy(3 - i // 2, r).start()
        return 0

    lax.fori_loop(0, tiles, phase_far, 0)
    head_out(tiles - 1)
    for u in range(2):
        half_p(u, far, 0).wait_send()

    def phase(t, _):
        k = 3 - t // tiles
        i = t % tiles
        q = tiles + 2 * t
        g_start(q + 2)
        g_wait(q)

        @pl.when(t >= 2)
        def _():
            full_p(t % 2, k, i).wait_send()

        psend[t % 2] = dot(slot_of(-k), 0, d, q).astype(BF16)
        full_p(t % 2, k, i).start()

        @pl.when(t < 4)
        def _():
            for u in range(2):
                transpose(2, 2 * t + u)

        g_start(q + 3)
        g_wait(q + 1)
        acc[...] = dot(slot_of(k), 0, d, q + 1)
        full_p(t % 2, k, i).wait_recv()

        @pl.when(k == 3)
        def _():
            rs_head(i).wait_recv()
            land[k, i, pl.ds(mine, half)] = (
                acc[pl.ds(mine, half)] + part[k - 1, i, pl.ds(mine, half)].astype(F32)
                + land[k, i, pl.ds(mine, half)].astype(F32)).astype(BF16)
            land[k, i, pl.ds(other, half)] = (
                acc[pl.ds(other, half)] + part[k - 1, i, pl.ds(other, half)].astype(F32)).astype(BF16)

        @pl.when(k < 3)
        def _():
            rs_full(k + 1, i).wait_recv()
            land[k, i] = (acc[...] + part[k - 1, i].astype(F32) + land[k, i].astype(F32)).astype(BF16)

        rs_full(k, i).start()
        return 0

    lax.fori_loop(0, 3 * tiles, phase, 0)
    for u in range(2):
        full_p(u, 1, 0).wait_send()

    def own_out(i):
        half_p(i % 2, 0, i).wait_recv()
        j = shard(0)
        out[j % mats, pl.ds(mine, half), columns(j, i)] = (
            acc[pl.ds(0, half)] + part_half[0, i].astype(F32)).astype(BF16)
        ag(1, i).start()
        across(0, i).start()

    def phase_own(i, _):
        q = 7 * tiles + i
        g_start(q + 2)
        g_wait(q)

        @pl.when(i >= 2)
        def _():
            half_p(i % 2, 0, i).wait_send()

        rs_full(1, i).wait_recv()
        psend[i % 2, pl.ds(0, half)] = (
            dot(0, other, half, q) + land[0, i, pl.ds(other, half)].astype(F32)).astype(BF16)
        half_p(i % 2, 0, i).start()

        @pl.when(i >= 1)
        def _():
            own_out(i - 1)

        acc[pl.ds(0, half)] = dot(0, mine, half, q) + land[0, i, pl.ds(mine, half)].astype(F32)
        return 0

    lax.fori_loop(0, tiles, phase_own, 0)
    own_out(tiles - 1)
    for u in range(2):
        half_p(u, 0, 0).wait_send()

    def gather(t, _):
        h = 1 + t // tiles
        i = t % tiles
        ag_arrival(h, i).wait_recv()

        @pl.when(h < chips - 1)
        def _():
            ag(h + 1, i).start()

        across(h, i).start()
        return 0

    lax.fori_loop(0, (chips - 1) * tiles, gather, 0)

    def drain(t, _):
        k = t // tiles
        i = t % tiles
        across_arrival(k, i).wait_recv()
        across(k, i).wait_send()

        @pl.when(k < chips - 1)
        def _():
            ag(k + 1, i).wait_send()

        @pl.when(k < 3)
        def _():
            rs_full(k + 1, i).wait_send()

        @pl.when(k == 3)
        def _():
            rs_head(i).wait_send()
        return 0

    lax.fori_loop(0, chips * tiles, drain, 0)


def store_kernel(x, o, sem):
    parts = [pltpu.make_async_copy(x.at[m], o.at[m], sem.at[m]) for m in range(x.shape[0])]
    for p in parts:
        p.start()
    for p in parts:
        p.wait()


def solution(mesh):
    n = mesh.shape["dp"]
    any_spec = pl.BlockSpec(memory_space=pl.ANY)
    vmem_spec = pl.BlockSpec(memory_space=pltpu.VMEM)

    def step(a, g):
        a, g = a[0], g[0]
        s = sizes(n, a.shape, g.shape)
        d, half, tile, tiles, chips = s["d"], s["half"], s["tile"], s["tiles"], s["chips"]
        shape = (s["mats"], d, s["ff"])
        dma = pltpu.SemaphoreType.DMA
        sums = pl.pallas_call(
            functools.partial(sum_kernel, n, s),
            name="sums",
            out_shape=pltpu.VMEM(shape, BF16),
            in_specs=[any_spec] * 2,
            out_specs=vmem_spec,
            scratch_shapes=[
                pltpu.VMEM((s["mats"], d, s["tokens"]), BF16),
                pltpu.VMEM((s["chunks"], s["chunk"], d), BF16),
                pltpu.VMEM((3, s["tokens"], tile), BF16),
                pltpu.VMEM((3, tiles, d, tile), BF16),
                pltpu.VMEM((2, tiles, half, tile), BF16),
                pltpu.VMEM((4, tiles, d, tile), BF16),
                pltpu.VMEM((tiles, half, tile), BF16),
                pltpu.VMEM((2, d, tile), BF16),
                pltpu.VMEM((d, tile), F32),
                dma((s["chunks"],)), dma((3,)), dma((2,)), dma((5, tiles)),
                dma((4, tiles)), dma((4, tiles)),
                dma((chips - 1, tiles)), dma((chips - 1, tiles)), dma((chips, tiles)), dma((chips, tiles)),
            ],
            compiler_params=pltpu.CompilerParams(
                collective_id=0, has_side_effects=True, vmem_limit_bytes=50 * 2**20),
        )(a, g)
        return pl.pallas_call(
            store_kernel,
            name="store",
            out_shape=jax.ShapeDtypeStruct(shape, BF16),
            in_specs=[vmem_spec],
            out_specs=any_spec,
            scratch_shapes=[dma((shape[0],))],
            compiler_params=pltpu.CompilerParams(vmem_limit_bytes=2**20),
        )(sums)

    return jax.shard_map(
        step, mesh=mesh, in_specs=(P(("rep", "dp")), P(("rep", "dp"))), out_specs=P("rep"), check_vma=False)
```

```python
import functools

import jax
import jax.numpy as jnp
from jax import lax
from jax.experimental import pallas as pl
from jax.experimental.pallas import tpu as pltpu
from jax.sharding import PartitionSpec as P

MESH = pl.DeviceIdType.MESH
F32 = jnp.float32
BF16 = jnp.bfloat16


def sizes(n, a_shape, g_shape):
    mats, tokens, d = a_shape
    ff = g_shape[2]
    chips = n // 2
    assert chips == 2 * mats and mats == 4
    width = ff * mats // chips
    tile = 256 if width % 256 == 0 else 128
    return dict(
        mats=mats, tokens=tokens, d=d, ff=ff, chips=chips, half=d // 2, width=width, tile=tile,
        tiles=width // tile, chunk=tokens // 16, chunks=16,
    )


def sum_kernel(n, s, a_hbm, g_hbm, out, at0, at1, at2, at3, araw, gbuf, part, part_half, land, psend, acc,
               a_sem, g_sem, g0_sem, ps_sem, pr_sem, rs_send, rs_recv, ag_send, ag_recv, ad_send, ad_recv):
    at = (at0, at1, at2, at3)
    ring = araw.shape[0]
    mats, chips, half, tile, tiles = s["mats"], s["chips"], s["half"], s["tile"], s["tiles"]
    d, width, chunk, chunks = s["d"], s["width"], s["chunk"], s["chunks"]
    far = chips // 2
    depth = gbuf.shape[0]
    me = lax.axis_index("dp")
    core = me % 2
    c = me // 2
    sgn = 2 * core - 1
    nxt = {"dp": ((c + sgn + chips) % chips) * 2 + core}
    prv = {"dp": ((c - sgn + chips) % chips) * 2 + core}
    partner = {"dp": c * 2 + 1 - core}
    mine = pl.multiple_of(core * half, half)
    other = pl.multiple_of((1 - core) * half, half)
    big = 8 * chips

    def shard(r):
        return (c + sgn * r + big) % chips

    def columns(j, i):
        return pl.ds(pl.multiple_of((j // mats) * width + i * tile, tile), tile)

    order = (0, 1, 3, 2)

    def a_copy(n):
        m = (c + sgn * order[n // chunks] + big) % mats
        return pltpu.make_async_copy(
            a_hbm.at[m, pl.ds(n % chunks * chunk, chunk)], araw.at[n % ring], a_sem.at[n % ring])

    def late(r):
        return (3 * chunks + r) % ring

    def late_copy(r):
        return pltpu.make_async_copy(a_hbm.at[0, pl.ds(0, chunk)], araw.at[late(r)], a_sem.at[late(r)])

    def transpose(n):
        at[order[n // chunks]][n % chunks] = araw[n % ring].T

    def g_copy(q, j, i):
        b = q % depth
        return pltpu.make_async_copy(g_hbm.at[j % mats, :, columns(j, i)], gbuf.at[b], g_sem.at[b])

    def g_start(q):
        @pl.when(q < tiles)
        def _():
            g_copy(q, shard(far), q).start()

        @pl.when((q >= tiles) & (q < tiles * 7))
        def _():
            r = q - tiles
            k = 3 - r // (2 * tiles)
            w = r % (2 * tiles)
            g_copy(q, shard(k * (2 * (w % 2) - 1)), w // 2).start()

        @pl.when((q >= tiles * 7) & (q < tiles * 8))
        def _():
            g_copy(q, shard(0), q - tiles * 7).start()

    def g_wait(q):
        g_copy(q, 0, 0).wait()

    def dot(slot, b, row, rows, t0=0, t1=chunks):
        lhs = jnp.concatenate([at[slot][t, pl.ds(row, rows), :] for t in range(t0, t1)], axis=1)
        return jnp.dot(lhs, gbuf[b, pl.ds(t0 * chunk, (t1 - t0) * chunk), :], preferred_element_type=F32)

    def dots(slot, q, t0=0, t1=chunks):
        return [dot(slot, q % depth, row, half, t0, t1) for row in (other, mine)]

    def held(i):
        return pl.ds(i % 2 * half, half)

    def to_partner(src, dst, u, k, i):
        return pltpu.make_async_remote_copy(
            src, dst, ps_sem.at[u], pr_sem.at[k, i], device_id=partner, device_id_type=MESH)

    def full_p(u, k, i):
        return to_partner(psend.at[u], part.at[k - 1, i], u, k, i)

    def half_p(u, k, i):
        return to_partner(psend.at[u, pl.ds(0, half)], part_half.at[k // far, i], u, k, i)

    def rs_head(i):
        return pltpu.make_async_remote_copy(
            part_half.at[1, i], land.at[far - 1, i, pl.ds(mine, half)], rs_send.at[far - 1, i],
            rs_recv.at[far - 1, i], device_id=nxt, device_id_type=MESH)

    def rs_full(k, i):
        return pltpu.make_async_remote_copy(
            land.at[k, i], land.at[k - 1, i], rs_send.at[k - 1, i], rs_recv.at[k - 1, i],
            device_id=nxt, device_id_type=MESH)

    def block(ref, j, row, i):
        return ref.at[j % mats, pl.ds(row, half), columns(j, i)]

    def ag(h, i):
        b = block(out, shard(-(h - 1)), mine, i)
        return pltpu.make_async_remote_copy(
            b, b, ag_send.at[h - 1, i], ag_recv.at[h - 1, i], device_id=nxt, device_id_type=MESH)

    def ag_arrival(h, i):
        b = block(out, shard(-h), mine, i)
        return pltpu.make_async_remote_copy(
            b, b, ag_send.at[h - 1, i], ag_recv.at[h - 1, i], device_id=nxt, device_id_type=MESH)

    def across(h, i):
        b = block(out, shard(-h), mine, i)
        return pltpu.make_async_remote_copy(
            b, b, ad_send.at[h, i], ad_recv.at[h, i], device_id=partner, device_id_type=MESH)

    def across_arrival(h, i):
        b = block(out, shard(h), other, i)
        return pltpu.make_async_remote_copy(
            b, b, ad_send.at[h, i], ad_recv.at[h, i], device_id=partner, device_id_type=MESH)

    def g_head(t):
        rows = pl.ds(t * chunk, chunk)
        j = shard(far)
        return pltpu.make_async_copy(g_hbm.at[j % mats, rows, columns(j, 0)], gbuf.at[0, rows], g0_sem.at[t])

    for t in range(chunks):
        a_copy(t).start()
        g_head(t).start()
    barrier = pltpu.get_barrier_semaphore()
    for peer in (nxt, prv, partner):
        pl.semaphore_signal(barrier, 1, device_id=peer, device_id_type=MESH)

    def head_out(i):
        half_p(i % 2, far, i).wait_recv()
        part_half[1, i] = (acc[held(i)] + part_half[1, i].astype(F32)).astype(BF16)
        rs_head(i).start()

    span = chunks // 4
    for t in range(0, chunks, span):
        for r in range(t, t + span):
            a_copy(r).wait()
            g_head(r).wait()
            transpose(r)
        if t == span:
            g_start(1)
        if t + span == chunks:
            for r in range(chunks, chunks + ring):
                a_copy(r).start()
            g_start(2)
        x, y = dots(0, 0, t, t + span)
        acc[held(1)] = x if t == 0 else acc[held(1)] + x
        acc[held(0)] = y if t == 0 else acc[held(0)] + y

    extras = ((), (), range(16, 30), range(30, 34), range(34, 48))
    for i in range(tiles):
        if i > 0:
            g_start(i + 2)
            for n_ in extras[i]:
                a_copy(n_).wait()
            g_wait(i)
            for n_ in extras[i]:
                transpose(n_)
            x, acc[held(i)] = dots(0, i)
        else:
            x = acc[held(1)]
        if i >= 2:
            half_p(i % 2, far, i).wait_send()
        psend[i % 2, pl.ds(0, half)] = x.astype(BF16)
        if i == 0:
            pl.semaphore_wait(barrier, 3)
        half_p(i % 2, far, i).start()
        if i >= 1:
            head_out(i - 1)
        for n_ in extras[i]:
            if n_ + ring < 4 * chunks:
                a_copy(n_ + ring).start()

    def phase(k, i, _):
        t = (3 - k) * tiles + i
        q = tiles + 2 * t

        def late_chunks(u):
            if k < 3:
                return
            for v in range(u, u + 2):
                r = 4 * (i - i // 4) + v

                @pl.when(i < 4)
                def _():
                    late_copy(r).wait()
            for v in range(u, u + 2):
                r = 4 * (i - i // 4) + v
                at2[r] = araw[late(r)].T

        g_start(q + 2)
        g_wait(q)
        late_chunks(0)
        x, y = dots(-k % mats, q)
        if k == 3:
            @pl.when(i < 2)
            def _():
                half_p(t % 2, far, i).wait_send()

        @pl.when(t >= 2)
        def _():
            full_p(t % 2, k, i).wait_send()

        psend[t % 2, pl.ds(other, half)] = x.astype(BF16)
        psend[t % 2, pl.ds(mine, half)] = y.astype(BF16)
        full_p(t % 2, k, i).start()
        if k == 3:
            @pl.when(i == 0)
            def _():
                head_out(tiles - 1)

        g_start(q + 3)
        g_wait(q + 1)
        late_chunks(2)
        acc[pl.ds(other, half)], acc[pl.ds(mine, half)] = dots(k % mats, q + 1)
        full_p(t % 2, k, i).wait_recv()
        (rs_head(i) if k == 3 else rs_full(k + 1, i)).wait_recv()
        for row in (other, mine):
            x = acc[pl.ds(row, half)] + part[k - 1, i, pl.ds(row, half)].astype(F32)
            if k < 3 or row is mine:
                x = x + land[k, i, pl.ds(row, half)].astype(F32)
            land[k, i, pl.ds(row, half)] = x.astype(BF16)
        rs_full(k, i).start()
        return 0

    for k in (3, 2, 1):
        lax.fori_loop(0, tiles, functools.partial(phase, k), 0)

    def own_out(i):
        half_p(i % 2, 0, i).wait_recv()
        j = shard(0)
        out[j % mats, pl.ds(mine, half), columns(j, i)] = (
            acc[held(i)] + land[0, i, pl.ds(mine, half)].astype(F32) + part_half[0, i].astype(F32)).astype(BF16)
        ag(1, i).start()
        across(0, i).start()

    def phase_own(i, _):
        q = 7 * tiles + i
        g_start(q + 2)
        g_wait(q)
        x, acc[held(i)] = dots(0, q)

        @pl.when(i < 2)
        def _():
            full_p(i % 2, 1, 0).wait_send()

        @pl.when(i >= 2)
        def _():
            half_p(i % 2, 0, i).wait_send()

        rs_full(1, i).wait_recv()
        psend[i % 2, pl.ds(0, half)] = (x + land[0, i, pl.ds(other, half)].astype(F32)).astype(BF16)
        half_p(i % 2, 0, i).start()

        @pl.when(i >= 1)
        def _():
            own_out(i - 1)

        return 0

    lax.fori_loop(0, tiles, phase_own, 0)
    own_out(tiles - 1)
    for u in range(2):
        half_p(u, 0, 0).wait_send()

    def gather(t, _):
        h = 1 + t // tiles
        i = t % tiles
        ag_arrival(h, i).wait_recv()

        @pl.when(h < chips - 1)
        def _():
            ag(h + 1, i).start()

        across(h, i).start()
        return 0

    lax.fori_loop(0, (chips - 1) * tiles, gather, 0)

    def drain(t, _):
        k = t // tiles
        i = t % tiles
        across_arrival(k, i).wait_recv()
        across(k, i).wait_send()

        @pl.when(k < chips - 1)
        def _():
            ag(k + 1, i).wait_send()

        @pl.when(k < 3)
        def _():
            rs_full(k + 1, i).wait_send()

        @pl.when(k == 3)
        def _():
            rs_head(i).wait_send()
        return 0

    lax.fori_loop(0, chips * tiles, drain, 0)


def store_kernel(x, o, sem):
    rows = x.shape[1] // 4
    blocks = [(m, pl.ds(r * rows, rows)) for m in range(x.shape[0]) for r in range(4)]
    parts = [pltpu.make_async_copy(x.at[b], o.at[b], sem.at[i]) for i, b in enumerate(blocks)]
    for p in parts:
        p.start()
    for p in parts:
        p.wait()


def solution(mesh):
    n = mesh.shape["dp"]
    any_spec = pl.BlockSpec(memory_space=pl.ANY)
    vmem_spec = pl.BlockSpec(memory_space=pltpu.VMEM)

    def step(a, g):
        a, g = a[0], g[0]
        s = sizes(n, a.shape, g.shape)
        d, half, tile, tiles, chips = s["d"], s["half"], s["tile"], s["tiles"], s["chips"]
        shape = (s["mats"], d, s["ff"])
        dma = pltpu.SemaphoreType.DMA
        sums = pl.pallas_call(
            functools.partial(sum_kernel, n, s),
            name="sums",
            out_shape=pltpu.VMEM(shape, BF16),
            in_specs=[any_spec] * 2,
            out_specs=vmem_spec,
            scratch_shapes=[
                *[pltpu.VMEM((s["chunks"], d, s["chunk"]), BF16) for _ in range(s["mats"])],
                pltpu.VMEM((18, s["chunk"], d), BF16),
                pltpu.VMEM((3, s["tokens"], tile), BF16),
                pltpu.VMEM((3, tiles, d, tile), BF16),
                pltpu.VMEM((2, tiles, half, tile), BF16),
                pltpu.VMEM((4, tiles, d, tile), BF16),
                pltpu.VMEM((2, d, tile), BF16),
                pltpu.VMEM((d, tile), F32),
                dma((18,)), dma((3,)), dma((s["chunks"],)), dma((2,)), dma((5, tiles)),
                dma((4, tiles)), dma((4, tiles)),
                dma((chips - 1, tiles)), dma((chips - 1, tiles)), dma((chips, tiles)), dma((chips, tiles)),
            ],
            compiler_params=pltpu.CompilerParams(
                collective_id=0, has_side_effects=True, vmem_limit_bytes=53_800_000),
        )(a, g)
        return pl.pallas_call(
            store_kernel,
            name="store",
            out_shape=jax.ShapeDtypeStruct(shape, BF16),
            in_specs=[vmem_spec],
            out_specs=any_spec,
            scratch_shapes=[dma((4 * shape[0],))],
            compiler_params=pltpu.CompilerParams(vmem_limit_bytes=2**20),
        )(sums)

    return jax.shard_map(
        step, mesh=mesh, in_specs=(P(("rep", "dp")), P(("rep", "dp"))), out_specs=P("rep"), check_vma=False)
```
